16 devices in a mesh: rep: 1, r: 4 (over y, z), s: 4 (over x, core).
Axes of the slice: x: 2, y: 2, z: 2, core: 2. Of those that a mesh axis runs over, the one named last changes fastest.
Arguments:
- x: bfloat16 [16, 4096, 1024], P(('rep', 'r', 's'))
- dy: bfloat16 [16, 4096, 1024], P(('rep', 'r', 's'))
- w_gate: bfloat16 [2, 1024, 4096], P(None, 's')
- w_up: bfloat16 [2, 1024, 4096], P(None, 's')
- w_down: bfloat16 [2, 4096, 1024], P(None, 's')
Outputs:
- output 1: bfloat16 [16, 4096, 1024], P(('rep', 'r', 's'))
- output 2: bfloat16 [2, 1024, 4096], P('rep', 's')
- output 3: bfloat16 [2, 1024, 4096], P('rep', 's')
- output 4: bfloat16 [2, 4096, 1024], P('rep', 's')
All inputs are finite; a program needn't handle non-finite values.
Results may differ from the reference program's by a relative error of at most 0.018.
Values are sent between devices in bfloat16 or wider.
A program may use at most 2 GiB of HBM per device.

```python
import jax
import jax.numpy as jnp
from jax import lax

SEQUENCES = 16
TOKENS = 4096
D = 1024
FF = 4096
LAYERS = 2
NAMES = ("w_gate", "w_up", "w_down")
SHAPES = {"w_gate": (LAYERS, D, FF), "w_up": (LAYERS, D, FF), "w_down": (LAYERS, FF, D)}


def bump(key, n, height):
    away = (jnp.arange(n, dtype=jnp.int32) - jax.random.randint(key, (), 0, n, jnp.int32)) % n
    return jnp.where(away < n // 8, height, 1.0)


def together(key, own, strength):
    shared = jax.random.normal(key, own.shape[1:], jnp.float32)
    return (own + strength * shared) * lax.rsqrt(1 + strength * strength)


def setup_inputs(seed: int = 0, part: int = 0) -> dict:
    kx, kdy, ka, kb, kz, kf, kh, kl, *kw = jax.random.split(jax.random.key(seed), 8 + len(NAMES))
    kx, kdy, ka, kb = (jax.random.fold_in(k, part) for k in (kx, kdy, ka, kb))
    shape = (SEQUENCES, TOKENS, D)
    much_x, much_dy = jax.random.uniform(kz, (2,), jnp.float32, 0.0, 1.0)
    layers = 2.0 ** jax.random.uniform(kl, (LAYERS, 1, 1), jnp.float32, -1.0, 1.0)
    x = together(ka, jax.random.normal(kx, shape, jnp.float32), much_x) * bump(kf, D, 4.0)
    dy = together(kb, jax.random.normal(kdy, shape, jnp.float32), much_dy)
    drawn = {"x": x.astype(jnp.bfloat16), "dy": (dy * (SEQUENCES * TOKENS) ** -0.5).astype(jnp.bfloat16)}
    for key, name in zip(kw, NAMES, strict=True):
        w = jax.random.normal(key, SHAPES[name], jnp.float32) * SHAPES[name][1] ** -0.5
        drawn[name] = (w * {"w_gate": 1.0, "w_up": bump(kh, FF, 4.0), "w_down": layers}[name]).astype(jnp.bfloat16)
    return drawn


def matmul(a, w):
    return jnp.dot(a, w, preferred_element_type=jnp.float32).astype(jnp.bfloat16)


def normed(h):
    wide = h.astype(jnp.float32)
    scale = lax.rsqrt(jnp.mean(wide**2, -1, keepdims=True) + 1e-6)
    return (wide * scale).astype(jnp.bfloat16)


def layer(h, w):
    a = normed(h)
    gate = jnp.dot(a, w["w_gate"], preferred_element_type=jnp.float32)
    up = jnp.dot(a, w["w_up"], preferred_element_type=jnp.float32)
    return h + matmul((jax.nn.silu(gate) * up).astype(jnp.bfloat16), w["w_down"])


def stack(weights, h):
    return lax.scan(lambda h, w: (layer(h, w), None), h, weights)[0]


def reference(x, dy, w_gate, w_up, w_down):
    weights = dict(zip(NAMES, (w_gate, w_up, w_down), strict=True))

    def take(so_far, sequence):
        h, by_y = sequence
        _, back = jax.vjp(stack, weights, h)
        by_weights, by_h = back(by_y)
        return jax.tree.map(lambda total, term: total + term.astype(jnp.float32), so_far, by_weights), by_h

    none_yet = {name: jnp.zeros(w.shape, jnp.float32) for name, w in weights.items()}
    by_weights, by_x = lax.scan(take, none_yet, (x, dy))
    return (by_x, *(by_weights[name].astype(jnp.bfloat16) for name in NAMES))
```

```python
import jax
import jax.numpy as jnp
from jax import lax
from jax.experimental import pallas as pl
from jax.experimental.pallas import tpu as pltpu
from jax.sharding import PartitionSpec as P

F32, BF = jnp.float32, jnp.bfloat16
LIMIT = 63_000_000
NN = (((1,), (0,)), ((), ()))
NT = (((1,), (1,)), ((), ()))
TN = (((0,), (0,)), ((), ()))


def dot(a, b, dims):
    return lax.dot_general(a, b, dims, preferred_element_type=F32)


def call(body, grid, ins, outs, shapes, flops, scratch=(), name=None):
    return pl.pallas_call(
        body,
        grid=grid,
        in_specs=ins,
        out_specs=outs,
        out_shape=shapes,
        scratch_shapes=list(scratch),
        compiler_params=pltpu.CompilerParams(vmem_limit_bytes=LIMIT, dimension_semantics=("arbitrary",) * len(grid)),
        cost_estimate=pl.CostEstimate(flops=flops, bytes_accessed=100_000_000, transcendentals=0),
        name=name,
    )


def scale_of(wide):
    return lax.rsqrt(jnp.mean(wide**2, -1, keepdims=True) + 1e-6)


def sds(shape, dtype=BF):
    return jax.ShapeDtypeStruct(shape, dtype)


def dgates(dh, g, u):
    s = jax.nn.sigmoid(g)
    dh = dh.astype(F32)
    silu = g * s
    return silu, (dh * u * (s * (1 + g * (1 - s)))).astype(BF), (dh * silu).astype(BF)


def gate_up(a, wg, wu, tm=512):
    t, d = a.shape
    c, _, tn = wg.shape
    f = c * tn

    def body(a_ref, wg_ref, wu_ref, h_ref, g_ref):
        a = a_ref[...]
        g = dot(a, wg_ref[0], NN)
        g_ref[...] = g
        u = dot(a, wu_ref[0], NN)
        h_ref[...] = (g * jax.nn.sigmoid(g) * u).astype(BF)

    w = pl.BlockSpec((1, d, tn), lambda j, i: (j, 0, 0))
    o = pl.BlockSpec((tm, tn), lambda j, i: (i, j))
    return call(body, (c, t // tm), [pl.BlockSpec((tm, d), lambda j, i: (i, 0)), w, w], [o, o],
                [sds((t, f)), sds((t, f), F32)], 4 * t * d * f, name="gate_up")(a, wg, wu)


def down(hidden, wd, h, tm=512):
    t, f = hidden.shape
    nr, ns, rows, d = wd.shape

    def body(hid_ref, wd_ref, h_ref, o_ref, a_ref):
        total = jnp.zeros((tm, d), F32)
        for s in range(ns):
            w = jnp.concatenate([wd_ref[r, s] for r in range(nr)], 0)
            total += dot(hid_ref[:, s * nr * rows:(s + 1) * nr * rows], w, NN)
        y = h_ref[...] + total.astype(BF)
        o_ref[...] = y
        wide = y.astype(F32)
        a_ref[...] = (wide * scale_of(wide)).astype(BF)

    r = pl.BlockSpec((tm, d), lambda i: (i, 0))
    return call(body, (t // tm,), [pl.BlockSpec((tm, f), lambda i: (i, 0)),
                pl.BlockSpec(wd.shape, lambda i: (0, 0, 0, 0), pipeline_mode=pl.Buffered(1)), r], [r, r],
                [sds((t, d)), sds((t, d))], 2 * t * d * f, name="down")(hidden, wd, h)


def mid(a, dy, wg, wu, wd, tm=512):
    t, d = a.shape
    c, _, tn = wg.shape
    f = c * tn
    nr, ns, rows, _ = wd.shape

    def body(a_ref, dy_ref, wg_ref, wu_ref, wd_ref, h_ref, dg_ref, du_ref):
        a = a_ref[...]
        g = dot(a, wg_ref[0], NN)
        u = dot(a, wu_ref[0], NN)
        dh = dot(dy_ref[...], wd_ref[...].reshape(tn, d), NT).astype(BF)
        silu, dg_ref[...], du_ref[...] = dgates(dh, g, u)
        h_ref[...] = (silu * u).astype(BF)

    r = pl.BlockSpec((tm, d), lambda j, i: (i, 0))
    w = pl.BlockSpec((1, d, tn), lambda j, i: (j, 0, 0))
    o = pl.BlockSpec((tm, tn), lambda j, i: (i, j))
    return call(body, (c, t // tm), [r, r, w, w, pl.BlockSpec((nr, 1, rows, d), lambda j, i: (0, j, 0, 0))], [o, o, o],
                [sds((t, f))] * 3, 6 * t * d * f, name="mid")(a, dy, wg, wu, wd)


def mid_saved(a, dy, g, wu, wd, tm=512):
    t, d = dy.shape
    c, _, tn = wu.shape
    f = c * tn
    nr, ns, rows, _ = wd.shape

    def body(a_ref, dy_ref, g_ref, wu_ref, wd_ref, dg_ref, du_ref):
        u = dot(a_ref[...], wu_ref[0], NN)
        dh = dot(dy_ref[...], wd_ref[...].reshape(tn, d), NT).astype(BF)
        _, dg_ref[...], du_ref[...] = dgates(dh, g_ref[...], u)

    r = pl.BlockSpec((tm, d), lambda j, i: (i, 0))
    w = pl.BlockSpec((1, d, tn), lambda j, i: (j, 0, 0))
    o = pl.BlockSpec((tm, tn), lambda j, i: (i, j))
    return call(body, (c, t // tm), [r, r, o, w, pl.BlockSpec((nr, 1, rows, d), lambda j, i: (0, j, 0, 0))], [o, o],
                [sds((t, f))] * 2, 4 * t * d * f, name="mid_saved")(a, dy, g, wu, wd)


def by_columns(a, q, nr=4, ns=4, tn=512):
    t, d = a.shape
    f = q.shape[1]
    rows = d // (nr * ns)

    def body(a_ref, q_ref, o_ref):
        w = dot(a_ref[...], q_ref[...], TN).astype(BF)
        for s in range(ns):
            for r in range(nr):
                o_ref[r, s] = w[(s * nr + r) * rows:(s * nr + r + 1) * rows]

    return call(body, (f // tn,), [pl.BlockSpec((t, d), lambda j: (0, 0), pipeline_mode=pl.Buffered(1)),
                pl.BlockSpec((t, tn), lambda j: (0, j))], pl.BlockSpec((nr, ns, rows, tn), lambda j: (0, 0, 0, j)),
                sds((nr, ns, rows, f)), 2 * t * d * f, name="by_columns")(a, q)


def by_rows(q, dy, nr=4, ns=4, tn=512):
    t, d = dy.shape
    f = q.shape[1]
    rows = f // (nr * ns)
    each = tn // rows
    per = nr // each

    def body(dy_ref, q_ref, o_ref):
        o_ref[...] = dot(q_ref[...], dy_ref[...], TN).astype(BF).reshape(o_ref.shape)

    return call(body, (f // tn,), [pl.BlockSpec((t, d), lambda j: (0, 0), pipeline_mode=pl.Buffered(1)),
                pl.BlockSpec((t, tn), lambda j: (0, j))],
                pl.BlockSpec((each, 1, rows, d), lambda j: (j % per, j // per, 0, 0)),
                sds((nr, ns, rows, d)), 2 * t * d * f, name="by_rows")(dy, q)


def back(dg, du, wg, wu, h, dy, tm=256):
    t, f = dg.shape
    c, d, tn = wg.shape

    def body(dg_ref, du_ref, wg_ref, wu_ref, h_ref, dy_ref, o_ref):
        def through(p_ref, w_ref):
            total = jnp.zeros((tm, d), F32)
            for j in range(c):
                total += dot(p_ref[:, j * tn:(j + 1) * tn], w_ref[j], NT)
            return total.astype(BF)
        da = (through(dg_ref, wg_ref) + through(du_ref, wu_ref)).astype(F32)
        wide = h_ref[...].astype(F32)
        scale = scale_of(wide)
        by = da * scale - wide * (scale**3 * jnp.mean(da * wide, -1, keepdims=True))
        o_ref[...] = dy_ref[...] + by.astype(BF)

    r = pl.BlockSpec((tm, d), lambda i: (i, 0))
    l = pl.BlockSpec((tm, f), lambda i: (i, 0))
    w = pl.BlockSpec((c, d, tn), lambda i: (0, 0, 0), pipeline_mode=pl.Buffered(1))
    return call(body, (t // tm,), [l, l, w, w, r, r], r, sds((t, d)), 4 * t * d * f, name="back")(dg, du, wg, wu, h, dy)


def normed(h):
    wide = h.astype(F32)
    return (wide * scale_of(wide)).astype(BF)


def solution(mesh):
    nr, ns = mesh.shape["r"], mesh.shape["s"]
    everyone = ("r", "s")

    def step(x, dy, w_gate, w_up, w_down):
        x, dy = x[0], dy[0]
        me = lax.axis_index("r")
        rows, f = w_gate.shape[1:]
        deep, d = w_down.shape[1:]

        def columns(w):
            return lax.dynamic_slice_in_dim(w, me * (f // nr), f // nr, 1)

        def wide(w):
            return w.reshape(nr, ns * rows, f // nr)

        def quarter(w):
            return lax.dynamic_slice_in_dim(w, me * (deep // nr), deep // nr, 0)

        def fetch(*ws):
            return [lax.all_gather(w, everyone, axis=0, tiled=True) for w in ws]

        def fetched(number):
            g, u, w = fetch(columns(w_gate[number]), columns(w_up[number]), quarter(w_down[number]))
            return wide(g), wide(u), w.reshape(nr, ns, deep // nr, d)

        g0, u0, d0 = fetched(0)
        g1, u1, d1 = fetched(1)
        a0 = normed(x)
        hidden0, gate0 = gate_up(a0, g0, u0)
        h1, a1 = down(hidden0, d0, x)
        hidden1, dg1, du1 = mid(a1, dy, g1, u1, d1)

        def reduced(term):
            flat = term.reshape((-1,) + term.shape[3:])
            return lax.psum_scatter(flat, everyone, scatter_dimension=0, tiled=True)

        down1 = reduced(by_rows(hidden1, dy))
        dh1 = back(dg1, du1, g1, u1, h1, dy)
        gate1 = reduced(by_columns(a1, dg1))
        up1 = reduced(by_columns(a1, du1))
        dg0, du0 = mid_saved(a0, dh1, gate0, u0, d0)
        down0 = reduced(by_rows(hidden0, dh1))
        gate0_ = reduced(by_columns(a0, dg0))
        up0 = reduced(by_columns(a0, du0))
        dx = back(dg0, du0, g0, u0, x, dh1)

        def whole(first, second):
            return jnp.stack([lax.all_gather(first, "r", axis=0, tiled=True), lax.all_gather(second, "r", axis=0, tiled=True)])

        return dx[None], whole(gate0_, gate1), whole(up0, up1), whole(down0, down1)

    states, cut = P(("rep", "r", "s"), None, None), P(None, "s", None)
    return jax.shard_map(
        step,
        mesh=mesh,
        in_specs=(states, states) + (cut,) * 3,
        out_specs=(states,) + (P("rep", "s", None),) * 3,
        check_vma=False,
    )
```

```python
import jax
import jax.numpy as jnp
from jax import lax
from jax.experimental import pallas as pl
from jax.experimental.pallas import tpu as pltpu
from jax.sharding import PartitionSpec as P

F32, BF = jnp.float32, jnp.bfloat16
LIMIT = 63_000_000
NN = (((1,), (0,)), ((), ()))
NT = (((1,), (1,)), ((), ()))
TN = (((0,), (0,)), ((), ()))


def dot(a, b, dims):
    return lax.dot_general(a, b, dims, preferred_element_type=F32)


def call(body, grid, ins, outs, shapes, flops, name, aliases={}, prefetch=0, scratch=()):
    return pl.pallas_call(
        body,
        grid_spec=pltpu.PrefetchScalarGridSpec(num_scalar_prefetch=prefetch, grid=grid, in_specs=ins, out_specs=outs,
                                              scratch_shapes=list(scratch)),
        out_shape=shapes,
        input_output_aliases=aliases,
        compiler_params=pltpu.CompilerParams(vmem_limit_bytes=LIMIT, dimension_semantics=("arbitrary",) * len(grid)),
        cost_estimate=pl.CostEstimate(flops=flops, bytes_accessed=100_000_000, transcendentals=0),
        name=name,
    )


def scale_of(wide):
    return lax.rsqrt(jnp.mean(wide**2, -1, keepdims=True) + 1e-6)


def normed(h):
    wide = h.astype(F32)
    return (wide * scale_of(wide)).astype(BF)


def sds(shape, dtype=BF):
    return jax.ShapeDtypeStruct(shape, dtype)


def once(shape, index):
    return pl.BlockSpec(shape, index, pipeline_mode=pl.Buffered(1))


def columns_of(w, which):
    nr, ns, _, rows, tn = w.shape
    return pl.BlockSpec((1, ns, 1, rows, tn), lambda j, i: (j, 0, which, 0, 0))


def rows_of(w, which):
    nr, ns, _, rows, d = w.shape
    return pl.BlockSpec((nr, 1, 1, rows, d), lambda j, i: (0, j, which, 0, 0))


def flat(w_ref):
    return w_ref[...].reshape(-1, w_ref.shape[-1])


def gate_up(a, w, tm=512):
    t, d = a.shape
    c, tn = w.shape[0], w.shape[-1]
    f = c * tn

    def body(a_ref, wg_ref, wu_ref, h_ref, g_ref):
        a = a_ref[...]
        g = dot(a, flat(wg_ref), NN)
        g_ref[...] = g
        u = dot(a, flat(wu_ref), NN)
        h_ref[...] = (g * jax.nn.sigmoid(g) * u).astype(BF)

    o = pl.BlockSpec((tm, tn), lambda j, i: (i, j))
    return call(body, (c, t // tm), [pl.BlockSpec((tm, d), lambda j, i: (i, 0)), columns_of(w, 0), columns_of(w, 1)], [o, o],
                [sds((t, f)), sds((t, f), F32)], 4 * t * d * f, "gate_up")(a, w, w)


def down(hidden, w, h, tm=512):
    t, f = hidden.shape
    nr, ns, _, rows, d = w.shape

    def body(hid_ref, w_ref, h_ref, o_ref, a_ref):
        total = jnp.zeros((tm, d), F32)
        for s in range(ns):
            block = jnp.concatenate([w_ref[r, s, 0] for r in range(nr)], 0)
            total += dot(hid_ref[:, s * nr * rows:(s + 1) * nr * rows], block, NN)
        y = h_ref[...] + total.astype(BF)
        o_ref[...] = y
        a_ref[...] = normed(y)

    r = pl.BlockSpec((tm, d), lambda i: (i, 0))
    return call(body, (t // tm,), [pl.BlockSpec((tm, f), lambda i: (i, 0)), once(w.shape, lambda i: (0, 0, 0, 0, 0)), r], [r, r],
                [sds((t, d)), sds((t, d))], 2 * t * d * f, "down")(hidden, w, h)


def dgates(dh, g, u):
    s = jax.nn.sigmoid(g)
    dh = dh.astype(F32)
    silu = g * s
    return silu, (dh * u * (s * (1 + g * (1 - s)))).astype(BF), (dh * silu).astype(BF)


def mid(a, dy, w, tm=512):
    t, d = a.shape
    c, tn = w.shape[0], w.shape[-1]
    f = c * tn

    def body(a_ref, dy_ref, wg_ref, wu_ref, wd_ref, h_ref, dgu_ref):
        a = a_ref[...]
        g = dot(a, flat(wg_ref), NN)
        u = dot(a, flat(wu_ref), NN)
        dh = dot(dy_ref[...], flat(wd_ref), NT).astype(BF)
        silu, dgu_ref[0], dgu_ref[1] = dgates(dh, g, u)
        h_ref[...] = (silu * u).astype(BF)

    r = pl.BlockSpec((tm, d), lambda j, i: (i, 0))
    return call(body, (c, t // tm), [r, r, columns_of(w, 0), columns_of(w, 1), rows_of(w, 2)],
                [pl.BlockSpec((tm, tn), lambda j, i: (i, j)), pl.BlockSpec((2, tm, tn), lambda j, i: (0, i, j))],
                [sds((t, f)), sds((2, t, f))], 6 * t * d * f, "mid")(a, dy, w, w, w)


def mid_saved(a, dy, g, w, wd, tm=512):
    t, d = dy.shape
    c, tn = w.shape[0], w.shape[-1]
    f = c * tn

    def body(a_ref, dy_ref, g_ref, wu_ref, wd_ref, dgu_ref):
        u = dot(a_ref[...], flat(wu_ref), NN)
        dh = dot(dy_ref[...], flat(wd_ref), NT).astype(BF)
        _, dgu_ref[0], dgu_ref[1] = dgates(dh, g_ref[...], u)

    r = pl.BlockSpec((tm, d), lambda j, i: (i, 0))
    return call(body, (c, t // tm), [r, r, pl.BlockSpec((tm, tn), lambda j, i: (i, j)), columns_of(w, 1), rows_of(wd, 0)],
                pl.BlockSpec((2, tm, tn), lambda j, i: (0, i, j)), sds((2, t, f)), 4 * t * d * f, "mid_saved")(a, dy, g, w, wd)


def by_columns(a, q, nr, ns, tn=1024):
    t, d = a.shape
    f = q.shape[-1]
    rows = d // (nr * ns)

    def body(a_ref, q_ref, o_ref):
        w = dot(a_ref[...], q_ref[0], TN).astype(BF)
        for s in range(ns):
            for r in range(nr):
                o_ref[r, s, 0] = w[(s * nr + r) * rows:(s * nr + r + 1) * rows]

    return call(body, (2, f // tn), [once((t, d), lambda k, j: (0, 0)), pl.BlockSpec((1, t, tn), lambda k, j: (k, 0, j))],
                pl.BlockSpec((nr, ns, 1, rows, tn), lambda k, j: (0, 0, k, 0, j)),
                sds((nr, ns, 2, rows, f)), 4 * t * d * f, "by_columns")(a, q)


def by_rows(q, dy, nr, ns, tn=512):
    t, d = dy.shape
    f = q.shape[1]
    rows = f // (nr * ns)
    each = tn // rows
    per = nr // each

    def body(dy_ref, q_ref, o_ref):
        o_ref[...] = dot(q_ref[...], dy_ref[...], TN).astype(BF).reshape(o_ref.shape)

    return call(body, (f // tn,), [once((t, d), lambda j: (0, 0)), pl.BlockSpec((t, tn), lambda j: (0, j))],
                pl.BlockSpec((each, 1, 1, rows, d), lambda j: (j % per, j // per, 0, 0, 0)),
                sds((nr, ns, 1, rows, d)), 2 * t * d * f, "by_rows")(dy, q)


def half_columns(where, a, q, nr, ns, added=None, tn=1024):
    t, d = a.shape
    f = q.shape[-1]
    wide = d // ns
    rows = wide // nr

    def body(where_ref, one_ref, two_ref, q_ref, *refs):
        total = refs[-1]
        for x, a_ref in enumerate((one_ref, two_ref)):
            total[x] = dot(a_ref[...], q_ref[0], TN)
        for place in range(nr):
            r = jnp.bitwise_xor(where_ref[2], place)
            for x in range(2):
                part = total[x, pl.ds(pl.multiple_of(r * rows, rows), rows)]
                if added is None:
                    refs[0][place, x, 0] = part.astype(BF)
                else:
                    refs[1 + 2 * place + x][0] = (part + refs[0][place, x, 0].astype(F32)).astype(BF)

    packed = pl.BlockSpec((nr, 2, 1, rows, tn), lambda k, j, b: (0, 0, k, 0, j))
    if added is None:
        more, o, shapes = (), packed, sds((nr, 2, 2, rows, f))
    else:
        more, o, shapes = (added,), [pl.BlockSpec((1, rows, tn), lambda k, j, b: (k, 0, j))] * (2 * nr), [sds((2, rows, f))] * (2 * nr)
    return call(body, (2, f // tn), [once((t, wide), lambda k, j, b: (0, b[0])), once((t, wide), lambda k, j, b: (0, b[1])),
                pl.BlockSpec((1, t, tn), lambda k, j, b: (k, 0, j))] + [packed] * len(more), o,
                shapes, 2 * t * d * f, "half_columns", prefetch=1, scratch=[pltpu.VMEM((2, wide, tn), F32)])(where, a, a, q, *more)


def back(q, w, h, dy, tm=256):
    _, t, f = q.shape
    c, ns, _, rows, tn = w.shape
    d = ns * rows

    def body(dg_ref, du_ref, wg_ref, wu_ref, h_ref, dy_ref, o_ref):
        def through(p_ref, w_ref):
            total = jnp.zeros((tm, d), F32)
            for j in range(c):
                total += dot(p_ref[0, :, j * tn:(j + 1) * tn], w_ref[j].reshape(d, tn), NT)
            return total.astype(BF)
        da = (through(dg_ref, wg_ref) + through(du_ref, wu_ref)).astype(F32)
        wide = h_ref[...].astype(F32)
        scale = scale_of(wide)
        by = da * scale - wide * (scale**3 * jnp.mean(da * wide, -1, keepdims=True))
        o_ref[...] = dy_ref[...] + by.astype(BF)

    def left(k):
        return pl.BlockSpec((1, tm, f), lambda i: (k, i, 0))

    def right(k):
        return once((c, ns, 1, rows, tn), lambda i: (0, 0, k, 0, 0))

    r = pl.BlockSpec((tm, d), lambda i: (i, 0))
    return call(body, (t // tm,), [left(0), left(1), right(0), right(1), r, r], r, sds((t, d)), 4 * t * d * f, "back")(q, q, w, w, h, dy)


def solution(mesh):
    nr, ns = mesh.shape["r"], mesh.shape["s"]
    everyone = ("r", "s")

    def swap(mask):
        return [(i, i ^ mask) for i in range(nr * ns)]

    def step(x, dy, w_gate, w_up, w_down):
        x, dy = x[0], dy[0]
        me, side, core = lax.axis_index("r"), lax.axis_index("s") // 2, lax.axis_index("s") % 2
        rows, f = w_gate.shape[1:]
        deep, d = w_down.shape[1:]

        def columns(w):
            return lax.dynamic_slice_in_dim(w, me * (f // nr), f // nr, 1)

        def quarter(w):
            return lax.dynamic_slice_in_dim(w, me * (deep // nr), deep // nr, 0)

        def gathered(*parts):
            sent = jnp.stack(parts)
            return lax.all_gather(sent, everyone, axis=0, tiled=False).reshape((nr, ns) + sent.shape)

        gu0 = gathered(columns(w_gate[0]), columns(w_up[0]))
        d0 = gathered(quarter(w_down[0]))
        all1 = gathered(columns(w_gate[1]), columns(w_up[1]), quarter(w_down[1]))
        a0 = normed(x)
        hidden0, gate0 = gate_up(a0, gu0)
        h1, a1 = down(hidden0, d0, x)

        def scattered(terms):
            return lax.psum_scatter(terms.reshape((nr * ns,) + terms.shape[2:]), everyone, scatter_dimension=0, tiled=False)

        def spread(own):
            return lax.all_gather(own, "r", axis=0, tiled=False)

        hidden1, q1 = mid(a1, dy, all1)
        down1 = scattered(by_rows(hidden1, dy, nr, ns))
        columns1, later = lax.optimization_barrier((by_columns(a1, q1, nr, ns), dy))
        up1 = scattered(columns1)
        dh1 = back(q1, all1, h1, later)
        rows0, later, down1 = lax.optimization_barrier((by_rows(hidden0, dh1, nr, ns), dh1, down1))
        down1, down0 = spread(down1), scattered(rows0)
        q0 = mid_saved(a0, later, gate0, gu0, d0)

        own, far = core + 2 * side, core + 2 * (1 - side)
        flip = 1 - 2 * core
        theirs = lax.ppermute(half_columns(jnp.stack([own + flip, far + flip, me]), a0, q0, nr, ns), everyone, swap(1))
        halves = half_columns(jnp.stack([own, far, me]), a0, q0, nr, ns, added=theirs)
        terms = [halves[0]] + [lax.ppermute(halves[place], everyone, swap(2 * place)) for place in range(1, 2 * nr)]
        last, up1, down0, terms[0] = lax.optimization_barrier((x, up1, down0, terms[0]))
        up1, down0 = spread(up1), spread(down0)
        dx = back(q0, gu0, last, dh1)
        dx, terms = lax.optimization_barrier((dx, terms))
        up0 = spread(sum(term.astype(F32) for term in terms).astype(BF))

        return (dx[None], *(jnp.stack([up0[:, k].reshape(rows, f), up1[:, k].reshape(rows, f)]) for k in (0, 1)),
                jnp.stack([down0.reshape(deep, d), down1.reshape(deep, d)]))

    states, cut = P(("rep", "r", "s"), None, None), P(None, "s", None)
    return jax.shard_map(
        step,
        mesh=mesh,
        in_specs=(states, states) + (cut,) * 3,
        out_specs=(states,) + (P("rep", "s", None),) * 3,
        check_vma=False,
    )
```

```python
import jax
import jax.numpy as jnp
from jax import lax
from jax.experimental import pallas as pl
from jax.experimental.pallas import tpu as pltpu
from jax.sharding import PartitionSpec as P

F32, BF = jnp.float32, jnp.bfloat16
LIMIT = 63_000_000
NN = (((1,), (0,)), ((), ()))
NT = (((1,), (1,)), ((), ()))
TN = (((0,), (0,)), ((), ()))


def dot(a, b, dims):
    return lax.dot_general(a, b, dims, preferred_element_type=F32)


def call(body, grid, ins, outs, shapes, flops, name, aliases={}, prefetch=0, scratch=()):
    return pl.pallas_call(
        body,
        grid_spec=pltpu.PrefetchScalarGridSpec(num_scalar_prefetch=prefetch, grid=grid, in_specs=ins, out_specs=outs,
                                              scratch_shapes=list(scratch)),
        out_shape=shapes,
        input_output_aliases=aliases,
        compiler_params=pltpu.CompilerParams(vmem_limit_bytes=LIMIT, dimension_semantics=("arbitrary",) * len(grid)),
        cost_estimate=pl.CostEstimate(flops=flops, bytes_accessed=100_000_000, transcendentals=0),
        name=name,
    )


def scale_of(wide):
    return lax.rsqrt(jnp.mean(wide**2, -1, keepdims=True) + 1e-6)


def normed(h):
    wide = h.astype(F32)
    return (wide * scale_of(wide)).astype(BF)


def sds(shape, dtype=BF):
    return jax.ShapeDtypeStruct(shape, dtype)


def once(shape, index):
    return pl.BlockSpec(shape, index, pipeline_mode=pl.Buffered(1))


def columns_of(w, which):
    nr, ns, _, rows, tn = w.shape
    return pl.BlockSpec((1, ns, 1, rows, tn), lambda j, i: (j, 0, which, 0, 0))


def rows_of(w, which):
    nr, ns, _, rows, d = w.shape
    return pl.BlockSpec((nr, 1, 1, rows, d), lambda j, i: (0, j, which, 0, 0))


def flat(w_ref):
    return w_ref[...].reshape(-1, w_ref.shape[-1])


def gate_up(a, w, tm=512):
    t, d = a.shape
    c, tn = w.shape[0], w.shape[-1]
    f = c * tn

    def body(a_ref, wg_ref, wu_ref, h_ref, g_ref):
        a = a_ref[...]
        g = dot(a, flat(wg_ref), NN)
        g_ref[...] = g
        u = dot(a, flat(wu_ref), NN)
        h_ref[...] = (g * jax.nn.sigmoid(g) * u).astype(BF)

    o = pl.BlockSpec((tm, tn), lambda j, i: (i, j))
    return call(body, (c, t // tm), [pl.BlockSpec((tm, d), lambda j, i: (i, 0)), columns_of(w, 0), columns_of(w, 1)], [o, o],
                [sds((t, f)), sds((t, f), F32)], 4 * t * d * f, "gate_up")(a, w, w)


def down(hidden, w, h, tm=512):
    t, f = hidden.shape
    nr, ns, _, rows, d = w.shape

    def body(hid_ref, w_ref, h_ref, o_ref, a_ref):
        total = jnp.zeros((tm, d), F32)
        for s in range(ns):
            block = jnp.concatenate([w_ref[r, s, 0] for r in range(nr)], 0)
            total += dot(hid_ref[:, s * nr * rows:(s + 1) * nr * rows], block, NN)
        y = h_ref[...] + total.astype(BF)
        o_ref[...] = y
        a_ref[...] = normed(y)

    r = pl.BlockSpec((tm, d), lambda i: (i, 0))
    return call(body, (t // tm,), [pl.BlockSpec((tm, f), lambda i: (i, 0)), once(w.shape, lambda i: (0, 0, 0, 0, 0)), r], [r, r],
                [sds((t, d)), sds((t, d))], 2 * t * d * f, "down")(hidden, w, h)


def dgates(dh, g, u):
    s = jax.nn.sigmoid(g)
    dh = dh.astype(F32)
    silu = g * s
    return silu, (dh * u * (s * (1 + g * (1 - s)))).astype(BF), (dh * silu).astype(BF)


def mid(a, dy, w, tm=512):
    t, d = a.shape
    c, tn = w.shape[0], w.shape[-1]
    f = c * tn

    def body(a_ref, dy_ref, wg_ref, wu_ref, wd_ref, h_ref, dgu_ref):
        a = a_ref[...]
        g = dot(a, flat(wg_ref), NN)
        u = dot(a, flat(wu_ref), NN)
        dh = dot(dy_ref[...], flat(wd_ref), NT).astype(BF)
        silu, dgu_ref[0], dgu_ref[1] = dgates(dh, g, u)
        h_ref[...] = (silu * u).astype(BF)

    r = pl.BlockSpec((tm, d), lambda j, i: (i, 0))
    return call(body, (c, t // tm), [r, r, columns_of(w, 0), columns_of(w, 1), rows_of(w, 2)],
                [pl.BlockSpec((tm, tn), lambda j, i: (i, j)), pl.BlockSpec((2, tm, tn), lambda j, i: (0, i, j))],
                [sds((t, f)), sds((2, t, f))], 6 * t * d * f, "mid")(a, dy, w, w, w)


def mid_saved(a, dy, g, w, wd, tm=512):
    t, d = dy.shape
    c, tn = w.shape[0], w.shape[-1]
    f = c * tn

    def body(a_ref, dy_ref, g_ref, wu_ref, wd_ref, dgu_ref):
        u = dot(a_ref[...], flat(wu_ref), NN)
        dh = dot(dy_ref[...], flat(wd_ref), NT).astype(BF)
        _, dgu_ref[0], dgu_ref[1] = dgates(dh, g_ref[...], u)

    r = pl.BlockSpec((tm, d), lambda j, i: (i, 0))
    return call(body, (c, t // tm), [r, r, pl.BlockSpec((tm, tn), lambda j, i: (i, j)), columns_of(w, 1), rows_of(wd, 0)],
                pl.BlockSpec((2, tm, tn), lambda j, i: (0, i, j)), sds((2, t, f)), 4 * t * d * f, "mid_saved")(a, dy, g, w, wd)


def by_columns(a, q, nr, ns, tn=1024):
    t, d = a.shape
    f = q.shape[-1]
    rows = d // (nr * ns)

    def body(a_ref, q_ref, o_ref):
        w = dot(a_ref[...], q_ref[0], TN).astype(BF)
        for s in range(ns):
            for r in range(nr):
                o_ref[r, s, 0] = w[(s * nr + r) * rows:(s * nr + r + 1) * rows]

    return call(body, (2, f // tn), [once((t, d), lambda k, j: (0, 0)), pl.BlockSpec((1, t, tn), lambda k, j: (k, 0, j))],
                pl.BlockSpec((nr, ns, 1, rows, tn), lambda k, j: (0, 0, k, 0, j)),
                sds((nr, ns, 2, rows, f)), 4 * t * d * f, "by_columns")(a, q)


def by_rows(q, dy, nr, ns, tn=512):
    t, d = dy.shape
    f = q.shape[1]
    rows = f // (nr * ns)
    each = tn // rows
    per = nr // each

    def body(dy_ref, q_ref, o_ref):
        o_ref[...] = dot(q_ref[...], dy_ref[...], TN).astype(BF).reshape(o_ref.shape)

    return call(body, (f // tn,), [once((t, d), lambda j: (0, 0)), pl.BlockSpec((t, tn), lambda j: (0, j))],
                pl.BlockSpec((each, 1, 1, rows, d), lambda j: (j % per, j // per, 0, 0, 0)),
                sds((nr, ns, 1, rows, d)), 2 * t * d * f, "by_rows")(dy, q)


def half_columns(where, a, q, nr, ns, added=None, tn=1024):
    t, d = a.shape
    f = q.shape[-1]
    wide = d // ns
    rows = wide // nr

    def body(where_ref, one_ref, two_ref, q_ref, *refs):
        total = refs[-1]
        for x, a_ref in enumerate((one_ref, two_ref)):
            total[x] = dot(a_ref[...], q_ref[0], TN)
        for place in range(nr):
            r = jnp.bitwise_xor(where_ref[2], place)
            for x in range(2):
                part = total[x, pl.ds(pl.multiple_of(r * rows, rows), rows)]
                if added is None:
                    refs[0][place, x, 0] = part.astype(BF)
                else:
                    refs[1 + 2 * place + x][0] = (part + refs[0][place, x, 0].astype(F32)).astype(BF)

    packed = pl.BlockSpec((nr, 2, 1, rows, tn), lambda k, j, b: (0, 0, k, 0, j))
    if added is None:
        more, o, shapes = (), packed, sds((nr, 2, 2, rows, f))
    else:
        more, o, shapes = (added,), [pl.BlockSpec((1, rows, tn), lambda k, j, b: (k, 0, j))] * (2 * nr), [sds((2, rows, f))] * (2 * nr)
    return call(body, (2, f // tn), [once((t, wide), lambda k, j, b: (0, b[0])), once((t, wide), lambda k, j, b: (0, b[1])),
                pl.BlockSpec((1, t, tn), lambda k, j, b: (k, 0, j))] + [packed] * len(more), o,
                shapes, 2 * t * d * f, "half_columns", prefetch=1, scratch=[pltpu.VMEM((2, wide, tn), F32)])(where, a, a, q, *more)


def back(q, w, h, dy, tm=256):
    _, t, f = q.shape
    c, ns, _, rows, tn = w.shape
    d = ns * rows

    def body(dg_ref, du_ref, wg_ref, wu_ref, h_ref, dy_ref, o_ref):
        def through(p_ref, w_ref):
            total = jnp.zeros((tm, d), F32)
            for j in range(c):
                total += dot(p_ref[0, :, j * tn:(j + 1) * tn], w_ref[j].reshape(d, tn), NT)
            return total.astype(BF)
        da = (through(dg_ref, wg_ref) + through(du_ref, wu_ref)).astype(F32)
        wide = h_ref[...].astype(F32)
        scale = scale_of(wide)
        by = da * scale - wide * (scale**3 * jnp.mean(da * wide, -1, keepdims=True))
        o_ref[...] = dy_ref[...] + by.astype(BF)

    def left(k):
        return pl.BlockSpec((1, tm, f), lambda i: (k, i, 0))

    def right(k):
        return once((c, ns, 1, rows, tn), lambda i: (0, 0, k, 0, 0))

    r = pl.BlockSpec((tm, d), lambda i: (i, 0))
    return call(body, (t // tm,), [left(0), left(1), right(0), right(1), r, r], r, sds((t, d)), 4 * t * d * f, "back")(q, q, w, w, h, dy)


def solution(mesh):
    nr, ns = mesh.shape["r"], mesh.shape["s"]
    everyone = ("r", "s")

    def swap(mask):
        return [(i, i ^ mask) for i in range(nr * ns)]

    def step(x, dy, w_gate, w_up, w_down):
        x, dy = x[0], dy[0]
        me, side, core = lax.axis_index("r"), lax.axis_index("s") // 2, lax.axis_index("s") % 2
        rows, f = w_gate.shape[1:]
        deep, d = w_down.shape[1:]

        def columns(w):
            return lax.dynamic_slice_in_dim(w, me * (f // nr), f // nr, 1)

        def quarter(w):
            return lax.dynamic_slice_in_dim(w, me * (deep // nr), deep // nr, 0)

        def gathered(*parts):
            sent = jnp.stack(parts)
            return lax.all_gather(sent, everyone, axis=0, tiled=False).reshape((nr, ns) + sent.shape)

        gu0 = gathered(columns(w_gate[0]), columns(w_up[0]))
        d0 = gathered(quarter(w_down[0]))
        all1 = gathered(columns(w_gate[1]), columns(w_up[1]), quarter(w_down[1]))
        a0 = normed(x)
        hidden0, gate0 = gate_up(a0, gu0)
        h1, a1 = down(hidden0, d0, x)

        def scattered(terms):
            return lax.psum_scatter(terms.reshape((nr * ns,) + terms.shape[2:]), everyone, scatter_dimension=0, tiled=False)

        def spread(own):
            return lax.all_gather(own, "r", axis=0, tiled=False)

        hidden1, q1 = mid(a1, dy, all1)
        down1 = scattered(by_rows(hidden1, dy, nr, ns))
        columns1, later = lax.optimization_barrier((by_columns(a1, q1, nr, ns), dy))
        up1 = scattered(columns1)
        dh1 = back(q1, all1, h1, later)
        rows0, later, down1 = lax.optimization_barrier((by_rows(hidden0, dh1, nr, ns), dh1, down1))
        down1 = spread(down1)
        q0 = mid_saved(a0, later, gate0, gu0, d0)
        rows0, q0, up1 = lax.optimization_barrier((rows0, q0, up1))
        down0 = scattered(rows0)

        own, far = core + 2 * side, core + 2 * (1 - side)
        flip = 1 - 2 * core
        theirs = lax.ppermute(half_columns(jnp.stack([own + flip, far + flip, me]), a0, q0, nr, ns), everyone, swap(1))
        halves = half_columns(jnp.stack([own, far, me]), a0, q0, nr, ns, added=theirs)
        terms = [halves[0]] + [lax.ppermute(halves[place], everyone, swap(2 * place)) for place in range(1, 2 * nr)]
        last, up1, down0, terms[0] = lax.optimization_barrier((x, up1, down0, terms[0]))
        up1, down0 = spread(up1), spread(down0)
        dx = back(q0, gu0, last, dh1)
        dx, terms = lax.optimization_barrier((dx, terms))
        up0 = spread(sum(term.astype(F32) for term in terms).astype(BF))

        return (dx[None], *(jnp.stack([up0[:, k].reshape(rows, f), up1[:, k].reshape(rows, f)]) for k in (0, 1)),
                jnp.stack([down0.reshape(deep, d), down1.reshape(deep, d)]))

    states, cut = P(("rep", "r", "s"), None, None), P(None, "s", None)
    return jax.shard_map(
        step,
        mesh=mesh,
        in_specs=(states, states) + (cut,) * 3,
        out_specs=(states,) + (P("rep", "s", None),) * 3,
        check_vma=False,
    )
```
